32 devices in a mesh: dp: 1 (over z), ff: 4 (over y), hd: 8 (over x, core).
Axes of the slice: x: 4, y: 4, z: 1, core: 2. Of those that a mesh axis runs over, the one named last changes fastest.
The devices are a block of a 4x4x8 slice.
Arguments:
- x_in: bfloat16 [512, 4096], P('dp', 'hd')
- w_up: bfloat16 [4096, 32768], P('hd', 'ff')
- b_up: float32 [32768], P('ff')
- w_down: bfloat16 [16384, 4096], P('ff', 'hd')
- b_down: float32 [4096], P('hd')
- ln_gain: float32 [4096], P('hd')
- ln_bias: float32 [4096], P('hd')
- dy_in: bfloat16 [512, 4096], P('dp', 'hd')
Outputs:
- output 1: bfloat16 [512, 4096], P('dp', 'hd')
- output 2: bfloat16 [512, 4096], P('dp', 'hd')
- output 3: float32 [4096, 32768], P(('dp', 'hd'), 'ff')
- output 4: float32 [16384, 4096], P(('dp', 'ff'), 'hd')
- output 5: float32 [32768], P(('dp', 'ff'))
- output 6: float32 [4096], P(('dp', 'hd'))
- output 7: float32 [4096], P(('dp', 'hd'))
- output 8: float32 [4096], P(('dp', 'hd'))
All inputs are finite; a program needn't handle non-finite values.
Results may differ from the reference program's by a relative error of at most 0.02.
Values are sent between devices in bfloat16 or wider.
A program may use at most 768 MiB of HBM per device.

```python
import math
import jax
import jax.numpy as jnp
from jax import lax

TOKENS = 512
HIDDEN = 4096
FFN = 16384
PAIR = 128
COARSE = 16
ALPHA = math.sqrt(140.0)
LN_EPS = 1e-5


def setup_inputs(seed: int = 0, part: int = 0) -> dict:
    part_keys = jax.random.split(jax.random.fold_in(jax.random.key(seed), part), 7)
    shared_keys = jax.random.split(jax.random.key(seed + 1), 6)
    seg_width = HIDDEN // COARSE
    row_shift = 0.7 * jax.random.normal(part_keys[0], (TOKENS, 1, 1), jnp.float32)
    seg_shift = 0.8 * jax.random.normal(part_keys[1], (1, COARSE, 1), jnp.float32)
    seg_scale = jnp.exp(0.4 * jax.random.normal(part_keys[2], (1, COARSE, 1), jnp.float32))
    x_noise = jax.random.normal(part_keys[3], (TOKENS, COARSE, seg_width), jnp.float32)
    x_vals = (row_shift + seg_shift + seg_scale * x_noise).reshape(TOKENS, HIDDEN)
    dy_noise = jax.random.normal(part_keys[4], (TOKENS, COARSE, seg_width), jnp.float32)
    dy_shift = 0.8 * jax.random.normal(part_keys[5], (TOKENS, 1, 1), jnp.float32)
    dy_tilt = jax.random.normal(part_keys[6], (TOKENS, 1, 1), jnp.float32)
    dy_vals = (dy_noise + dy_shift + dy_tilt * seg_shift).reshape(TOKENS, HIDDEN)
    w_up = jax.random.normal(shared_keys[0], (HIDDEN, 2 * FFN), jnp.float32) * HIDDEN ** -0.5
    b_up = 0.5 * jax.random.normal(shared_keys[1], (2 * FFN,), jnp.float32)
    w_down = jax.random.normal(shared_keys[2], (FFN, HIDDEN), jnp.float32) * (ALPHA * FFN ** -0.5)
    b_down = 3.0 * jax.random.normal(shared_keys[3], (HIDDEN,), jnp.float32)
    ln_gain = 1.0 + 0.3 * jax.random.normal(shared_keys[4], (HIDDEN,), jnp.float32)
    ln_bias = 0.3 * jax.random.normal(shared_keys[5], (HIDDEN,), jnp.float32)
    return {'x_in': x_vals.astype(jnp.bfloat16), 'w_up': w_up.astype(jnp.bfloat16), 'b_up': b_up, 'w_down': w_down.astype(jnp.bfloat16), 'b_down': b_down, 'ln_gain': ln_gain, 'ln_bias': ln_bias, 'dy_in': dy_vals.astype(jnp.bfloat16)}


def gelu_tanh(z_val):
    return jax.nn.gelu(z_val, approximate=True)


def reference(x_in, w_up, b_up, w_down, b_down, ln_gain, ln_bias, dy_in):
    n_blocks = FFN // PAIR
    u_acc = jnp.dot(x_in, w_up, preferred_element_type=jnp.float32) + b_up
    u_act = u_acc.astype(jnp.bfloat16).reshape(TOKENS, n_blocks, 2, PAIR)
    val_half = u_act[:, :, 0, :].astype(jnp.float32)
    gate_half = u_act[:, :, 1, :].astype(jnp.float32)
    gelu_out, gelu_vjp = jax.vjp(gelu_tanh, gate_half)
    m_act = (val_half * gelu_out).astype(jnp.bfloat16).reshape(TOKENS, FFN)
    f_out = jnp.dot(m_act, w_down, preferred_element_type=jnp.float32)
    residual = ALPHA * x_in.astype(jnp.float32) + f_out + b_down
    row_mean = jnp.mean(residual, axis=1, keepdims=True)
    centered = residual - row_mean
    row_var = jnp.mean(centered * centered, axis=1, keepdims=True)
    inv_std = lax.rsqrt(row_var + LN_EPS)
    normed = centered * inv_std
    y_out = (ln_gain * normed + ln_bias).astype(jnp.bfloat16)
    dy_f = dy_in.astype(jnp.float32)
    g_dy = dy_f * ln_gain
    d_resid = inv_std * (g_dy - jnp.mean(g_dy, axis=1, keepdims=True) - normed * jnp.mean(g_dy * normed, axis=1, keepdims=True))
    dr_b = d_resid.astype(jnp.bfloat16)
    d_mact = jnp.dot(dr_b, w_down.T, preferred_element_type=jnp.float32).reshape(TOKENS, n_blocks, PAIR)
    d_val = d_mact * gelu_out
    d_gate = gelu_vjp(d_mact * val_half)[0]
    du_f = jnp.stack([d_val, d_gate], axis=2).reshape(TOKENS, 2 * FFN)
    du_b = du_f.astype(jnp.bfloat16)
    dw_up = jnp.dot(x_in.T, du_b, preferred_element_type=jnp.float32)
    dw_down = jnp.dot(m_act.T, dr_b, preferred_element_type=jnp.float32)
    dx_out = (ALPHA * d_resid + jnp.dot(du_b, w_up.T, preferred_element_type=jnp.float32)).astype(jnp.bfloat16)
    return (y_out, dx_out, dw_up, dw_down, jnp.sum(du_f, axis=0), jnp.sum(d_resid, axis=0), jnp.sum(dy_f * normed, axis=0), jnp.sum(dy_f, axis=0))
```

```python
import functools
import math
import jax
import jax.numpy as jnp
from jax import lax
from jax.experimental import pallas as pl
from jax.experimental.pallas import tpu as pltpu
from jax.sharding import PartitionSpec as P

PAIR = 128
ALPHA = math.sqrt(140.0)
LN_EPS = 1e-5
CORES = 2
NCHUNK = 2
F32 = jnp.float32
BF16 = jnp.bfloat16
MESH = pl.DeviceIdType.MESH
GELU_C = math.sqrt(2.0 / math.pi)
GELU_A = 0.044715


def dot_nn(a, b):
    return lax.dot_general(a, b, (((1,), (0,)), ((), ())), preferred_element_type=F32)


def dot_nt(a, b):
    return lax.dot_general(a, b, (((1,), (1,)), ((), ())), preferred_element_type=F32)


def dot_tn(a, b):
    return lax.dot_general(a, b, (((0,), (0,)), ((), ())), preferred_element_type=F32)


def mlp_kernel(cfg, x_hbm, w1_hbm, b1_ref, w2_hbm, b2_ref, gam_ref, bet_ref, dy_hbm,
               y_out, d_out, m_out, du_out, dxp_out, drq_out, db1_out, small_out,
               xo, xx, dyv, w1v, w1x, w2v, w2x,
               ps1, rf1, rn1, own1, ps2, rf2, rn2, own2, uo, mb, dub,
               facc, fs, fr, rbuf, drq, st, do, dx, yv, dbuf, cs, csr, dxacc, dxs,
               s_sem, r_sem, l_sem):
    nff, nhd, T, HL, UH, FB = cfg
    nx = nhd // CORES
    FH = FB // 2
    TC = T // NCHUNK
    TQ = TC // nff
    hidden = HL * nhd
    h_me = lax.axis_index("hd")
    y_me = lax.axis_index("ff")
    x_me = lax.div(h_me, CORES)
    c_me = lax.rem(h_me, CORES)
    c_ot = 1 - c_me

    def xdev(off):
        return {"hd": lax.rem(x_me + off, nx) * CORES + c_me}

    XP, XM = xdev(1), xdev(nx - 1)
    CO = {"hd": x_me * CORES + c_ot}

    def ydev(s):
        return {"ff": lax.rem(y_me + s, nff)}

    def hdev(s):
        return {"hd": lax.rem(h_me + s, nhd)}

    def quarter(off):
        return lax.rem(x_me + off, nx)

    def block(off):
        return c_me * nx + quarter(off)

    b_own = block(0)

    bar = pltpu.get_barrier_semaphore()
    for s in range(1, nhd):
        pl.semaphore_signal(bar, inc=1, device_id=hdev(s), device_id_type=MESH)
    for s in range(1, nff):
        pl.semaphore_signal(bar, inc=1, device_id=ydev(s), device_id_type=MESH)

    cnt = {"r": 0, "l": 0}
    sent = []
    D = {}

    def rsend(name, src, dst, dev):
        i = cnt["r"]
        cnt["r"] += 1
        cp = pltpu.make_async_remote_copy(src_ref=src, dst_ref=dst, send_sem=s_sem.at[i], recv_sem=r_sem.at[i],
                                          device_id=dev, device_id_type=MESH)
        cp.start()
        sent.append(cp)
        D[name] = cp

    def rwait(name):
        D[name].wait_recv()

    def lcopy(name, src, dst):
        i = cnt["l"]
        cnt["l"] += 1
        cp = pltpu.make_async_copy(src, dst, l_sem.at[i])
        cp.start()
        D[name] = cp

    def lwait(name):
        D[name].wait()

    order = (2, 1, nx - 1, 0)
    lcopy("x", x_hbm, xo)

    def load_half(b, h):
        return w1_hbm.at[:, pl.ds(pl.multiple_of((2 * b + h) * UH, UH), UH)]

    for j, off in enumerate(order):
        for h in range(2):
            lcopy(("w1", j, h), load_half(block(off), h), w1v.at[2 * block(off) + h])
    lcopy("dy", dy_hbm, dyv)
    lcopy("w2", w2_hbm, w2v)
    pl.semaphore_wait(bar, nhd - 1 + nff - 1)
    rsend("xx", x_hbm, xx, CO)
    for j, off in enumerate(order):
        for h in range(2):
            q = quarter(off)
            rsend(("w1x", j, h), load_half(c_ot * nx + q, h), w1x.at[2 * q + h], CO)
    rsend("w2x", w2_hbm.at[pl.ds(c_ot * nx, nx)], w2x, CO)
    for q in range(nx):
        for h in range(2):
            b = c_ot * nx + q
            lcopy(("w1o", q, h), load_half(b, h), w1v.at[2 * b + h])

    def rows(k):
        return pl.ds(k * TC, TC)

    def rs_first(tag, k, j, ps, rf, rn):
        if j == 0:
            rsend((tag, "fA", k), ps.at[0, 0, rows(k)], rf.at[0, rows(k)], XP)
            rsend((tag, "fB", k), ps.at[0, 1, rows(k)], rf.at[1, rows(k)], XM)
        elif j == 1:
            rsend((tag, "nB", k), ps.at[1, 1, rows(k)], rn.at[0, 1, rows(k)], XP)
        elif j == 2:
            rsend((tag, "nA", k), ps.at[2, 0, rows(k)], rn.at[1, 0, rows(k)], XM)

    def rs_combine(tag, k, ps, rf, rn):
        for d, (nm, out, j, h, dev) in enumerate((("fA", "cA", 1, 0, XP), ("fB", "cB", 2, 1, XM))):
            rwait((tag, nm, k))
            ps[j, h, rows(k)] = (ps[j, h, rows(k)].astype(F32) + rf[d, rows(k)].astype(F32)).astype(BF16)
            rsend((tag, out, k), ps.at[j, h, rows(k)], rn.at[d, h, rows(k)], dev)

    def rs_wait(tag, k):
        for nm in ("nB", "nA", "cA", "cB"):
            rwait((tag, nm, k))

    def ag_first(tag, k, view):
        for nm, dev in (("p", XP), ("m", XM), ("o0", CO)):
            rsend((tag, nm, k), view(b_own, rows(k)), view(b_own, rows(k)), dev)

    def ag_forward(tag, k, view):
        half = TC // 2
        ra, rb = pl.ds(k * TC, half), pl.ds(k * TC + half, half)
        bm, bp = block(nx - 1), block(1)
        rwait((tag, "p", k))
        rsend((tag, "fA", k), view(bm, ra), view(bm, ra), XP)
        rsend((tag, "o1", k), view(bm, rows(k)), view(bm, rows(k)), CO)
        rwait((tag, "m", k))
        rsend((tag, "fB", k), view(bp, rb), view(bp, rb), XM)
        rsend((tag, "o2", k), view(bp, rows(k)), view(bp, rows(k)), CO)

    def ag_last(tag, k, view):
        bf = block(2)
        rwait((tag, "fA", k))
        rwait((tag, "fB", k))
        rsend((tag, "o3", k), view(bf, rows(k)), view(bf, rows(k)), CO)
        for i in range(4):
            rwait((tag, "o%d" % i, k))

    def m_view(b, r):
        return mb.at[b, r]

    def du_view(b, r):
        return dub.at[pl.ds(2 * b, 2), r]

    def u_partial(k):
        for j, off in enumerate(order):
            for h in range(2):
                if k == 0:
                    lwait(("w1", j, h))
                    rwait(("w1x", j, h))
            b, q = block(off), quarter(off)

            @pl.loop(0, 2)
            def _(h):
                p = dot_nn(xo[rows(k)], w1v[2 * b + h]) + dot_nn(xx[rows(k)], w1x[2 * q + h])
                if j < 3:
                    ps1[j, h, rows(k)] = p.astype(BF16)
                else:
                    own1[h, rows(k)] = p

            if k == 0:
                rs_first("U", k, j, ps1, rf1, rn1)

    def u_send(k):
        for j in range(3):
            rs_first("U", k, j, ps1, rf1, rn1)

    TS = 32

    def activate(k):
        rs_wait("U", k)
        bias = b1_ref[pl.ds(b_own, 1), :]

        @pl.loop(0, TC // TS)
        def _(i):
            r = pl.ds(pl.multiple_of(k * TC + i * TS, TS), TS)
            for h in range(2):
                u = own1[h, r] + rn1[0, h, r].astype(F32) + rn1[1, h, r].astype(F32)
                u = (u + bias[:, h * UH:(h + 1) * UH]).astype(BF16)
                uo[h, r] = u
                for p in range(UH // (2 * PAIR)):
                    v = u[:, 2 * p * PAIR:(2 * p + 1) * PAIR].astype(F32)
                    g = u[:, (2 * p + 1) * PAIR:(2 * p + 2) * PAIR].astype(F32)
                    t = jnp.tanh(GELU_C * (g + GELU_A * (g * g * g)))
                    m = v * (g * (0.5 * (1.0 + t)))
                    lo = h * FH + p * PAIR
                    mb[b_own, r, lo:lo + PAIR] = m.astype(BF16)

        ag_first("M", k, m_view)

    def f_partial(k):
        ag_last("M", k, m_view)
        lcopy(("mo", k), mb.at[:, rows(k)], m_out.at[:, rows(k)])
        facc[k] = jnp.zeros_like(facc[k])
        if k == 0:
            lwait("w2")

        @pl.loop(0, nhd)
        def _(b):
            facc[k] += dot_nn(mb[b, rows(k)], w2v[b])

        fs[rows(k)] = facc[k].astype(BF16)
        for s in range(1, nff):
            yy = lax.rem(y_me + s, nff)
            rsend(("f", s, k), fs.at[pl.ds(pl.multiple_of(k * TC + yy * TQ, TQ), TQ)], fr.at[k, s - 1], ydev(s))

    def q_rows(k, yy):
        return pl.ds(pl.multiple_of(k * TC + yy * TQ, TQ), TQ)

    def ln_stats(k):
        if k == 0:
            lwait("dy")
        for s in range(1, nff):
            rwait(("f", s, k))
        r = facc[k, pl.ds(pl.multiple_of(y_me * TQ, TQ), TQ)]
        for s in range(1, nff):
            r = r + fr[k, s - 1].astype(F32)
        r = ALPHA * xo[q_rows(k, y_me)].astype(F32) + r + b2_ref[0:1, :]
        rbuf[k] = r
        g = dyv[q_rows(k, y_me)].astype(F32) * gam_ref[0:1, :]
        mean = jnp.sum(r, axis=1, keepdims=True) * (1.0 / HL)
        rc = r - mean
        m2 = jnp.sum(rc * rc, axis=1, keepdims=True)
        gs = jnp.sum(g, axis=1, keepdims=True)
        gc = jnp.sum(g * rc, axis=1, keepdims=True)
        lane = lax.broadcasted_iota(jnp.int32, (TQ, 128), 1)
        cols = jnp.where(lane == 0, mean, jnp.where(lane == 1, m2, jnp.where(lane == 2, gs, jnp.where(lane == 3, gc, 0.0))))
        full = jnp.concatenate([cols, jnp.zeros((128 - TQ, 128), F32)], axis=0) if TQ < 128 else cols
        st[k, h_me] = full.T[0:8, :]
        for s in range(1, nhd):
            rsend(("st", s, k), st.at[k, h_me], st.at[k, h_me], hdev(s))

    def ln_apply(k):
        for s in range(1, nhd):
            rwait(("st", s, k))
        mean_sum = jnp.zeros((1, 128), F32)
        for i in range(nhd):
            mean_sum = mean_sum + st[k, i, 0:1, :]
        mu = mean_sum * (1.0 / nhd)
        ss = jnp.zeros((1, 128), F32)
        gs = jnp.zeros((1, 128), F32)
        gr = jnp.zeros((1, 128), F32)
        for i in range(nhd):
            dev = st[k, i, 0:1, :] - mu
            ss = ss + st[k, i, 1:2, :] + HL * (dev * dev)
            gs = gs + st[k, i, 2:3, :]
            gr = gr + st[k, i, 3:4, :] + dev * st[k, i, 2:3, :]
        rho = lax.rsqrt(ss * (1.0 / hidden) + LN_EPS)
        gm = gs * (1.0 / hidden)
        grm = rho * gr * (1.0 / hidden)
        row = lax.broadcasted_iota(jnp.int32, (128, 128), 0)
        z = jnp.where(row == 0, mu, jnp.where(row == 1, rho, jnp.where(row == 2, gm, jnp.where(row == 3, grm, 0.0))))
        z = z.T[0:TQ, :]
        mu, rho, gm, grm = z[:, 0:1], z[:, 1:2], z[:, 2:3], z[:, 3:4]
        normed = (rbuf[k] - mu) * rho
        qr = q_rows(k, y_me)
        dyq = dyv[qr].astype(F32)
        g = dyq * gam_ref[0:1, :]
        dr = rho * (g - gm - normed * grm)
        drq[k] = dr
        do[qr] = dr.astype(BF16)
        for s in range(1, nff):
            rsend(("d", s, k), do.at[qr], do.at[qr], ydev(s))
        rsend(("dc", 0, k), do.at[qr], dx.at[qr], CO)
        yv[qr] = (gam_ref[0:1, :] * normed + bet_ref[0:1, :]).astype(BF16)
        for s in range(1, nff):
            rsend(("y", s, k), yv.at[qr], yv.at[qr], ydev(s))
        cs[0:1, :] += jnp.sum(dr, axis=0, keepdims=True)
        cs[1:2, :] += jnp.sum(dyq * normed, axis=0, keepdims=True)

    def d_forward(k):
        for s in range(1, nff):
            rwait(("d", s, k))
            qr = q_rows(k, lax.rem(y_me + nff - s, nff))
            rsend(("dc", s, k), do.at[qr], dx.at[qr], CO)

    def dm_partial(k):
        if k == 0:
            rwait("w2x")
        for s in range(nff):
            rwait(("dc", s, k))
        for j, off in enumerate(order):
            b, q = block(off), quarter(off)
            p = dot_nt(do[rows(k)], w2v[b]) + dot_nt(dx[rows(k)], w2x[q])
            for h in range(2):
                ph = p[:, h * FH:(h + 1) * FH]
                if j < 3:
                    ps2[j, h, rows(k)] = ph.astype(BF16)
                else:
                    own2[h, rows(k)] = ph
            rs_first("G", k, j, ps2, rf2, rn2)

    def du_make(k):
        rs_wait("G", k)

        @pl.loop(0, TC // TS)
        def _(i):
            r = pl.ds(pl.multiple_of(k * TC + i * TS, TS), TS)
            for h in range(2):
                dm = own2[h, r] + rn2[0, h, r].astype(F32) + rn2[1, h, r].astype(F32)
                u = uo[h, r]
                for p in range(UH // (2 * PAIR)):
                    v = u[:, 2 * p * PAIR:(2 * p + 1) * PAIR].astype(F32)
                    g = u[:, (2 * p + 1) * PAIR:(2 * p + 2) * PAIR].astype(F32)
                    dmp = dm[:, p * PAIR:(p + 1) * PAIR]
                    gg = g * g
                    t = jnp.tanh(GELU_C * (g + GELU_A * (gg * g)))
                    cdf = 0.5 * (1.0 + t)
                    dv = dmp * (g * cdf)
                    slope = cdf + (0.5 * g) * (1.0 - t * t) * (GELU_C * (1.0 + 3.0 * GELU_A * gg))
                    dg = dmp * v * slope
                    lo = 2 * p * PAIR
                    dub[2 * b_own + h, r, lo:lo + PAIR] = dv.astype(BF16)
                    dub[2 * b_own + h, r, lo + PAIR:lo + 2 * PAIR] = dg.astype(BF16)
                    sl = h * (UH // PAIR) + 2 * p
                    dbuf[b_own, sl:sl + 1, :] += jnp.sum(dv, axis=0, keepdims=True)
                    dbuf[b_own, sl + 1:sl + 2, :] += jnp.sum(dg, axis=0, keepdims=True)

        ag_first("V", k, du_view)

    def dx_partial(k):
        ag_last("V", k, du_view)
        lcopy(("duo", k), dub.at[:, rows(k)], du_out.at[:, rows(k)])
        dxacc[...] = jnp.zeros_like(dxacc)
        if k == 0:
            for q in range(nx):
                for h in range(2):
                    lwait(("w1o", q, h))

        @pl.loop(0, 2 * nhd)
        def _(i):
            dxacc[...] += dot_nt(dub[i, rows(k)], w1v[i])

        dxs[rows(k)] = dxacc[...].astype(BF16)
        lcopy(("dxo", k), dxs.at[rows(k)], dxp_out.at[rows(k)])

    cs[...] = jnp.zeros_like(cs)
    dbuf[b_own] = jnp.zeros_like(dbuf[b_own])
    lwait("x")
    rwait("xx")
    u_partial(0)
    u_partial(1)
    rs_combine("U", 0, ps1, rf1, rn1)
    u_send(1)
    activate(0)
    rs_combine("U", 1, ps1, rf1, rn1)
    ag_forward("M", 0, m_view)
    activate(1)
    f_partial(0)
    ag_forward("M", 1, m_view)
    ln_stats(0)
    ln_apply(0)
    f_partial(1)
    d_forward(0)
    ln_stats(1)
    dm_partial(0)
    ln_apply(1)
    rs_combine("G", 0, ps2, rf2, rn2)
    for s in range(1, nff):
        rsend(("cs", s), cs, csr.at[s - 1], ydev(s))
    d_forward(1)
    du_make(0)
    dm_partial(1)
    ag_forward("V", 0, du_view)
    rs_combine("G", 1, ps2, rf2, rn2)
    du_make(1)
    for s in range(1, nhd):
        rsend(("db", s), dbuf.at[b_own], dbuf.at[b_own], hdev(s))
    dx_partial(0)
    ag_forward("V", 1, du_view)
    lcopy("do", do, d_out)
    lcopy("dro", drq, drq_out)
    for k in range(NCHUNK):
        for s in range(1, nff):
            rwait(("y", s, k))
    lcopy("yo", yv, y_out)
    tot = cs[...]
    for s in range(1, nff):
        rwait(("cs", s))
        tot = tot + csr[s - 1]
    small_out[0:2, :] = tot[0:2, :]
    small_out[2:3, :] = jnp.sum(dyv[...].astype(F32), axis=0, keepdims=True)
    small_out[3:8, :] = jnp.zeros((5, HL), F32)
    for s in range(1, nhd):
        rwait(("db", s))
    db1_out[...] = dbuf[...]
    dx_partial(1)
    for nm in ("do", "dro", "yo"):
        lwait(nm)
    for k in range(NCHUNK):
        for nm in ("mo", "duo", "dxo"):
            lwait((nm, k))
    for cp in sent:
        cp.wait_send()


def comm_call(mesh, x, w1, b1, w2, b2, gam, bet, dy):
    nff, nhd = mesh.shape['ff'], mesh.shape['hd']
    T, HL = x.shape
    UH = w1.shape[1] // (2 * nhd)
    FB = w2.shape[0] // nhd
    FH = FB // 2
    TC = T // NCHUNK
    TQ = TC // nff
    nx = nhd // CORES
    V = pltpu.VMEM
    scratch = [
        V((T, HL), BF16), V((T, HL), BF16), V((T, HL), BF16),
        V((2 * nhd, HL, UH), BF16), V((2 * nx, HL, UH), BF16), V((nhd, FB, HL), BF16), V((nx, FB, HL), BF16),
        V((3, 2, T, UH), BF16), V((2, T, UH), BF16), V((2, 2, T, UH), BF16), V((2, T, UH), F32),
        V((3, 2, T, FH), BF16), V((2, T, FH), BF16), V((2, 2, T, FH), BF16), V((2, T, FH), F32),
        V((2, T, UH), BF16), V((nhd, T, FB), BF16), V((2 * nhd, T, UH), BF16),
        V((NCHUNK, TC, HL), F32), V((T, HL), BF16), V((NCHUNK, nff - 1, TQ, HL), BF16),
        V((NCHUNK, TQ, HL), F32), V((NCHUNK, TQ, HL), F32), V((NCHUNK, nhd, 8, 128), F32),
        V((T, HL), BF16), V((T, HL), BF16), V((T, HL), BF16),
        V((nhd, 2 * UH // 128, 128), F32), V((8, HL), F32), V((nff - 1, 8, HL), F32),
        V((TC, HL), F32), V((T, HL), BF16),
        pltpu.SemaphoreType.DMA((160,)), pltpu.SemaphoreType.DMA((160,)), pltpu.SemaphoreType.DMA((40,)),
    ]
    anyspec = pl.BlockSpec(memory_space=pl.ANY)
    vspec = pl.BlockSpec(memory_space=pltpu.VMEM)
    S = jax.ShapeDtypeStruct
    return pl.pallas_call(
        functools.partial(mlp_kernel, (nff, nhd, T, HL, UH, FB)),
        out_shape=[S((T, HL), BF16), S((T, HL), BF16), S((nhd, T, FB), BF16), S((2 * nhd, T, UH), BF16),
                   S((T, HL), BF16), S((NCHUNK, TQ, HL), F32), S((nhd, 2 * UH // 128, 128), F32), S((8, HL), F32)],
        in_specs=[anyspec, anyspec, vspec, anyspec, vspec, vspec, vspec, anyspec],
        out_specs=[anyspec, anyspec, anyspec, anyspec, anyspec, anyspec, vspec, vspec],
        scratch_shapes=scratch,
        compiler_params=pltpu.CompilerParams(collective_id=0, has_side_effects=True, vmem_limit_bytes=67043328),
        name="mlp_comm",
    )(x, w1, b1.reshape(nhd, 2 * UH), w2.reshape(nhd, FB, HL), b2.reshape(1, HL), gam.reshape(1, HL), bet.reshape(1, HL), dy)


def dw2_kernel(m_ref, d_ref, o_ref):
    o_ref[...] = dot_tn(m_ref[0], d_ref[...])


def dw1_kernel(x_ref, du_ref, o_ref):
    o_ref[...] = dot_tn(x_ref[...], du_ref[0])


def weight_grads(x, d, m, du):
    n2, T, FB = m.shape
    n1, _, UH = du.shape
    HL = x.shape[1]
    dw2 = pl.pallas_call(
        dw2_kernel, grid=(n2,), out_shape=jax.ShapeDtypeStruct((n2 * FB, HL), F32),
        in_specs=[pl.BlockSpec((1, T, FB), lambda i: (i, 0, 0)), pl.BlockSpec((T, HL), lambda i: (0, 0))],
        out_specs=pl.BlockSpec((FB, HL), lambda i: (i, 0)),
        cost_estimate=pl.CostEstimate(flops=2 * n2 * FB * HL * T, bytes_accessed=n2 * FB * HL * 4 + n2 * FB * T * 2, transcendentals=0),
        name="dw2",
    )(m, d)
    dw1 = pl.pallas_call(
        dw1_kernel, grid=(n1,), out_shape=jax.ShapeDtypeStruct((HL, n1 * UH), F32),
        in_specs=[pl.BlockSpec((T, HL), lambda i: (0, 0)), pl.BlockSpec((1, T, UH), lambda i: (i, 0, 0))],
        out_specs=pl.BlockSpec((HL, UH), lambda i: (0, i)),
        cost_estimate=pl.CostEstimate(flops=2 * n1 * UH * HL * T, bytes_accessed=n1 * UH * HL * 4 + n1 * UH * T * 2, transcendentals=0),
        name="dw1",
    )(x, du)
    return dw1, dw2


def solution(mesh):
    nff = mesh.shape['ff']
    data_spec = P('dp', 'hd')
    hid_spec = P('hd')
    in_specs = (data_spec, P('hd', 'ff'), P('ff'), P('ff', 'hd'), hid_spec, hid_spec, hid_spec, data_spec)
    out_specs = (data_spec, data_spec, P(('dp', 'hd'), 'ff'), P(('dp', 'ff'), 'hd'), P(('dp', 'ff')), P(('dp', 'hd')), P(('dp', 'hd')), P(('dp', 'hd')))

    def shift(v, s):
        return lax.ppermute(v, 'ff', [(i, (i + s) % nff) for i in range(nff)])

    def device_step(x_loc, w_up, b_up, w_down, b_down, ln_gain, ln_bias, dy_loc):
        T, HL = x_loc.shape
        y_loc, d_loc, m_all, du_all, dxp, drq, db1, small = comm_call(
            mesh, x_loc, w_up, b_up, w_down, b_down, ln_gain, ln_bias, dy_loc)
        y_me = lax.axis_index('ff')
        TQ = T // (NCHUNK * nff)
        parts = dxp.reshape(NCHUNK, nff, TQ, HL)

        def part(s):
            return lax.dynamic_index_in_dim(parts, lax.rem(y_me + s, nff), axis=1, keepdims=False)

        got = [shift(part(s), s) for s in range(1, nff)]
        dw_up, dw_down = weight_grads(x_loc, d_loc, m_all, du_all)
        acc = part(0).astype(F32)
        for v in got:
            acc = acc + v.astype(F32)
        mine = (ALPHA * drq + acc).astype(BF16)
        out = jnp.zeros((NCHUNK, nff, TQ, HL), BF16)
        out = lax.dynamic_update_index_in_dim(out, mine, y_me, axis=1)
        for s in range(1, nff):
            out = lax.dynamic_update_index_in_dim(out, shift(mine, s), lax.rem(y_me + nff - s, nff), axis=1)
        dx_loc = out.reshape(T, HL)
        return (y_loc, dx_loc, dw_up, dw_down, db1.reshape(-1), small[0], small[1], small[2])

    return jax.shard_map(device_step, mesh=mesh, in_specs=in_specs, out_specs=out_specs, check_vma=False)
```

```python
import functools
import math
import jax
import jax.numpy as jnp
from jax import lax
from jax.experimental import pallas as pl
from jax.experimental.pallas import tpu as pltpu
from jax.sharding import PartitionSpec as P

PAIR = 128
ALPHA = math.sqrt(140.0)
LN_EPS = 1e-5
CORES = 2
NCHUNK = 2
F32 = jnp.float32
BF16 = jnp.bfloat16
MESH = pl.DeviceIdType.MESH
GELU_C = math.sqrt(2.0 / math.pi)
GELU_A = 0.044715


def dot_nn(a, b):
    return lax.dot_general(a, b, (((1,), (0,)), ((), ())), preferred_element_type=F32)


def dot_nt(a, b):
    return lax.dot_general(a, b, (((1,), (1,)), ((), ())), preferred_element_type=F32)


def dot_tn(a, b):
    return lax.dot_general(a, b, (((0,), (0,)), ((), ())), preferred_element_type=F32)


def mlp_kernel(cfg, x_hbm, w1_hbm, b1_ref, w2_hbm, b2_ref, gam_ref, bet_ref, dy_hbm,
               y_out, d_out, mt_out, du_out, dx_out, xt_out, db1_out, small_out,
               xo, xx, dyv, w1v, w1x, w2v, w2x,
               ps1, rf1, rn1, own1, ps2, rf2, rn2, own2, uo, mb, dub,
               facc, fs, fr, rbuf, drq, st, do, dx, yv, dbuf, cs, csr, dxacc, dxs, dxr, dxv, mt, xt,
               s_sem, r_sem, l_sem):
    nff, nhd, T, HL, UH, FB = cfg
    nx = nhd // CORES
    FH = FB // 2
    TC = T // NCHUNK
    TQ = TC // nff
    hidden = HL * nhd
    h_me = lax.axis_index("hd")
    y_me = lax.axis_index("ff")
    x_me = lax.div(h_me, CORES)
    c_me = lax.rem(h_me, CORES)
    c_ot = 1 - c_me

    def xdev(off):
        return {"hd": lax.rem(x_me + off, nx) * CORES + c_me}

    XP, XM = xdev(1), xdev(nx - 1)
    CO = {"hd": x_me * CORES + c_ot}

    def ydev(s):
        return {"ff": lax.rem(y_me + s, nff)}

    def hdev(s):
        return {"hd": lax.rem(h_me + s, nhd)}

    def quarter(off):
        return lax.rem(x_me + off, nx)

    def block(off):
        return c_me * nx + quarter(off)

    b_own = block(0)

    bar = pltpu.get_barrier_semaphore()
    for s in range(1, nhd):
        pl.semaphore_signal(bar, inc=1, device_id=hdev(s), device_id_type=MESH)
    for s in range(1, nff):
        pl.semaphore_signal(bar, inc=1, device_id=ydev(s), device_id_type=MESH)

    cnt = {"r": 0, "l": 0}
    sent = []
    D = {}

    def rsend(name, src, dst, dev):
        i = cnt["r"]
        cnt["r"] += 1
        cp = pltpu.make_async_remote_copy(src_ref=src, dst_ref=dst, send_sem=s_sem.at[i], recv_sem=r_sem.at[i],
                                          device_id=dev, device_id_type=MESH)
        cp.start()
        sent.append(cp)
        D[name] = cp

    def rwait(name):
        D[name].wait_recv()

    def lcopy(name, src, dst):
        i = cnt["l"]
        cnt["l"] += 1
        cp = pltpu.make_async_copy(src, dst, l_sem.at[i])
        cp.start()
        D[name] = cp

    def lwait(name):
        D[name].wait()

    order = (2, 1, nx - 1, 0)
    lcopy("x", x_hbm, xo)

    def load_half(b, h):
        return w1_hbm.at[:, pl.ds(pl.multiple_of((2 * b + h) * UH, UH), UH)]

    for j, off in enumerate(order):
        for h in range(2):
            lcopy(("w1", j, h), load_half(block(off), h), w1v.at[2 * block(off) + h])
    lcopy("dy", dy_hbm, dyv)
    lcopy("w2", w2_hbm, w2v)
    pl.semaphore_wait(bar, nhd - 1 + nff - 1)
    rsend("xx", x_hbm, xx, CO)

    def push_w1(j):
        q = quarter(order[j])
        for h in range(2):
            rsend(("w1x", j, h), load_half(c_ot * nx + q, h), w1x.at[2 * q + h], CO)

    for j in range(3):
        push_w1(j)
    for q in range(nx):
        for h in range(2):
            b = c_ot * nx + q
            lcopy(("w1o", q, h), load_half(b, h), w1v.at[2 * b + h])

    def rows(k):
        return pl.ds(k * TC, TC)

    def rs_first(tag, k, j, ps, rf, rn, only=None):
        for h in (0, 1) if only is None else (only,):
            if j == 0 and h == 0:
                rsend((tag, "fA", k), ps.at[0, 0, rows(k)], rf.at[0, rows(k)], XP)
            elif j == 0:
                rsend((tag, "fB", k), ps.at[0, 1, rows(k)], rf.at[1, rows(k)], XM)
            elif j == 1 and h == 1:
                rsend((tag, "nB", k), ps.at[1, 1, rows(k)], rn.at[0, 1, rows(k)], XP)
            elif j == 2 and h == 0:
                rsend((tag, "nA", k), ps.at[2, 0, rows(k)], rn.at[1, 0, rows(k)], XM)

    def rs_combine(tag, k, ps, rf, rn):
        for d, (nm, out, j, h, dev) in enumerate((("fA", "cA", 1, 0, XP), ("fB", "cB", 2, 1, XM))):
            rwait((tag, nm, k))
            ps[j, h, rows(k)] = (ps[j, h, rows(k)].astype(F32) + rf[d, rows(k)].astype(F32)).astype(BF16)
            rsend((tag, out, k), ps.at[j, h, rows(k)], rn.at[d, h, rows(k)], dev)

    def rs_wait(tag, k):
        for nm in ("nB", "nA", "cA", "cB"):
            rwait((tag, nm, k))

    def ag_first(tag, k, view):
        for nm, dev in (("p", XP), ("m", XM), ("o0", CO)):
            rsend((tag, nm, k), view(b_own, rows(k)), view(b_own, rows(k)), dev)

    def ag_forward(tag, k, view):
        half = TC // 2
        ra, rb = pl.ds(k * TC, half), pl.ds(k * TC + half, half)
        bm, bp = block(nx - 1), block(1)
        rwait((tag, "p", k))
        rsend((tag, "fA", k), view(bm, ra), view(bm, ra), XP)
        rsend((tag, "o1", k), view(bm, rows(k)), view(bm, rows(k)), CO)
        rwait((tag, "m", k))
        rsend((tag, "fB", k), view(bp, rb), view(bp, rb), XM)
        rsend((tag, "o2", k), view(bp, rows(k)), view(bp, rows(k)), CO)

    def oblock(off):
        return c_ot * nx + quarter(off)

    def ag_last(tag, k, view, use):
        for off in (0, nx - 1, 1):
            use(block(off))
        for i, off in ((0, 0), (1, nx - 1), (2, 1)):
            rwait((tag, "o%d" % i, k))
            use(oblock(off))
        bf = block(2)
        rwait((tag, "fA", k))
        rwait((tag, "fB", k))
        rsend((tag, "o3", k), view(bf, rows(k)), view(bf, rows(k)), CO)
        use(bf)
        rwait((tag, "o3", k))
        use(oblock(2))

    def m_view(b, r):
        return mb.at[b, r]

    def du_view(b, r):
        return dub.at[pl.ds(2 * b, 2), r]

    def u_partial(k):
        for j, off in enumerate(order):
            b, q = block(off), quarter(off)

            def half(h):
                p = dot_nn(xo[rows(k)], w1v[2 * b + h]) + dot_nn(xx[rows(k)], w1x[2 * q + h])
                if j < 3:
                    ps1[j, h, rows(k)] = p.astype(BF16)
                else:
                    own1[h, rows(k)] = p

            if k > 0:
                pl.loop(0, 2)(half)
            else:
                for h in ((1, 0) if j == 1 else (0, 1)):
                    lwait(("w1", j, h))
                    rwait(("w1x", j, h))
                    half(h)
                    rs_first("U", k, j, ps1, rf1, rn1, h)
                if j == 1:
                    push_w1(3)
                    rsend("w2x", w2_hbm.at[pl.ds(c_ot * nx, nx)], w2x, CO)

    def u_send(k, js):
        for j in js:
            rs_first("U", k, j, ps1, rf1, rn1)

    TS = 32

    def activate(k):
        rs_wait("U", k)
        bias = b1_ref[b_own]
        nsl = UH // PAIR

        @pl.loop(0, TC // TS)
        def _(i):
            r = pl.ds(pl.multiple_of(k * TC + i * TS, TS), TS)
            for h in range(2):
                u = own1[h, r] + rn1[0, h, r].astype(F32) + rn1[1, h, r].astype(F32)
                u = jnp.concatenate([u[:, p * PAIR:(p + 1) * PAIR] + bias[h * nsl + p:h * nsl + p + 1, :] for p in range(nsl)], axis=1)
                u = u.astype(BF16)
                uo[h, r] = u
                for p in range(UH // (2 * PAIR)):
                    v = u[:, 2 * p * PAIR:(2 * p + 1) * PAIR].astype(F32)
                    g = u[:, (2 * p + 1) * PAIR:(2 * p + 2) * PAIR].astype(F32)
                    t = jnp.tanh(GELU_C * (g + GELU_A * (g * g * g)))
                    m = v * (g * (0.5 * (1.0 + t)))
                    lo = h * FH + p * PAIR
                    mb[b_own, r, lo:lo + PAIR] = m.astype(BF16)

        ag_first("M", k, m_view)

    def f_partial(k):
        facc[k] = jnp.zeros_like(facc[k])
        if k == 0:
            lwait("w2")

        def use(b):
            facc[k] += dot_nn(mb[b, rows(k)], w2v[b])

        ag_last("M", k, m_view, use)
        fs[rows(k)] = facc[k].astype(BF16)
        for s in range(1, nff):
            yy = lax.rem(y_me + s, nff)
            rsend(("f", s, k), fs.at[pl.ds(pl.multiple_of(k * TC + yy * TQ, TQ), TQ)], fr.at[k, s - 1], ydev(s))

    def q_rows(k, yy):
        return pl.ds(pl.multiple_of(k * TC + yy * TQ, TQ), TQ)

    def ln_stats(k):
        if k == 0:
            lwait("dy")
        for s in range(1, nff):
            rwait(("f", s, k))
        r = facc[k, pl.ds(pl.multiple_of(y_me * TQ, TQ), TQ)]
        for s in range(1, nff):
            r = r + fr[k, s - 1].astype(F32)
        r = ALPHA * xo[q_rows(k, y_me)].astype(F32) + r + b2_ref[0:1, :]
        rbuf[k] = r
        g = dyv[q_rows(k, y_me)].astype(F32) * gam_ref[0:1, :]
        mean = jnp.sum(r, axis=1, keepdims=True) * (1.0 / HL)
        rc = r - mean
        m2 = jnp.sum(rc * rc, axis=1, keepdims=True)
        gs = jnp.sum(g, axis=1, keepdims=True)
        gc = jnp.sum(g * rc, axis=1, keepdims=True)
        lane = lax.broadcasted_iota(jnp.int32, (TQ, 128), 1)
        cols = jnp.where(lane == 0, mean, jnp.where(lane == 1, m2, jnp.where(lane == 2, gs, jnp.where(lane == 3, gc, 0.0))))
        full = jnp.concatenate([cols, jnp.zeros((128 - TQ, 128), F32)], axis=0) if TQ < 128 else cols
        st[k, h_me] = full.T[0:8, :]
        for s in range(1, nhd):
            rsend(("st", s, k), st.at[k, h_me], st.at[k, h_me], hdev(s))

    def ln_apply(k):
        for s in range(1, nhd):
            rwait(("st", s, k))
        mean_sum = jnp.zeros((1, 128), F32)
        for i in range(nhd):
            mean_sum = mean_sum + st[k, i, 0:1, :]
        mu = mean_sum * (1.0 / nhd)
        ss = jnp.zeros((1, 128), F32)
        gs = jnp.zeros((1, 128), F32)
        gr = jnp.zeros((1, 128), F32)
        for i in range(nhd):
            dev = st[k, i, 0:1, :] - mu
            ss = ss + st[k, i, 1:2, :] + HL * (dev * dev)
            gs = gs + st[k, i, 2:3, :]
            gr = gr + st[k, i, 3:4, :] + dev * st[k, i, 2:3, :]
        rho = lax.rsqrt(ss * (1.0 / hidden) + LN_EPS)
        gm = gs * (1.0 / hidden)
        grm = rho * gr * (1.0 / hidden)
        row = lax.broadcasted_iota(jnp.int32, (128, 128), 0)
        z = jnp.where(row == 0, mu, jnp.where(row == 1, rho, jnp.where(row == 2, gm, jnp.where(row == 3, grm, 0.0))))
        z = z.T[0:TQ, :]
        mu, rho, gm, grm = z[:, 0:1], z[:, 1:2], z[:, 2:3], z[:, 3:4]
        normed = (rbuf[k] - mu) * rho
        qr = q_rows(k, y_me)
        dyq = dyv[qr].astype(F32)
        g = dyq * gam_ref[0:1, :]
        dr = rho * (g - gm - normed * grm)
        drq[k] = dr
        do[qr] = dr.astype(BF16)
        for s in range(1, nff):
            rsend(("d", s, k), do.at[qr], do.at[qr], ydev(s))
        rsend(("dc", 0, k), do.at[qr], dx.at[qr], CO)
        yv[qr] = (gam_ref[0:1, :] * normed + bet_ref[0:1, :]).astype(BF16)
        for s in range(1, nff):
            rsend(("y", s, k), yv.at[qr], yv.at[qr], ydev(s))
        cs[0:1, :] += jnp.sum(dr, axis=0, keepdims=True)
        cs[1:2, :] += jnp.sum(dyq * normed, axis=0, keepdims=True)

    def d_forward(k):
        for s in range(1, nff):
            rwait(("d", s, k))
            qr = q_rows(k, lax.rem(y_me + nff - s, nff))
            rsend(("dc", s, k), do.at[qr], dx.at[qr], CO)

    def dm_partial(k):
        if k == 0:
            rwait("w2x")
        for s in range(nff):
            rwait(("dc", s, k))
        for j, off in enumerate(order):
            b, q = block(off), quarter(off)
            p = dot_nt(do[rows(k)], w2v[b]) + dot_nt(dx[rows(k)], w2x[q])
            for h in range(2):
                ph = p[:, h * FH:(h + 1) * FH]
                if j < 3:
                    ps2[j, h, rows(k)] = ph.astype(BF16)
                else:
                    own2[h, rows(k)] = ph
            rs_first("G", k, j, ps2, rf2, rn2)

    def du_make(k):
        rs_wait("G", k)

        @pl.loop(0, TC // TS)
        def _(i):
            r = pl.ds(pl.multiple_of(k * TC + i * TS, TS), TS)
            for h in range(2):
                dm = own2[h, r] + rn2[0, h, r].astype(F32) + rn2[1, h, r].astype(F32)
                u = uo[h, r]
                for p in range(UH // (2 * PAIR)):
                    v = u[:, 2 * p * PAIR:(2 * p + 1) * PAIR].astype(F32)
                    g = u[:, (2 * p + 1) * PAIR:(2 * p + 2) * PAIR].astype(F32)
                    dmp = dm[:, p * PAIR:(p + 1) * PAIR]
                    gg = g * g
                    t = jnp.tanh(GELU_C * (g + GELU_A * (gg * g)))
                    cdf = 0.5 * (1.0 + t)
                    dv = dmp * (g * cdf)
                    slope = cdf + (0.5 * g) * (1.0 - t * t) * (GELU_C * (1.0 + 3.0 * GELU_A * gg))
                    dg = dmp * v * slope
                    lo = 2 * p * PAIR
                    dub[2 * b_own + h, r, lo:lo + PAIR] = dv.astype(BF16)
                    dub[2 * b_own + h, r, lo + PAIR:lo + 2 * PAIR] = dg.astype(BF16)
                    sl = h * (UH // PAIR) + 2 * p
                    dbuf[b_own, sl:sl + 1, :] += jnp.sum(dv, axis=0, keepdims=True)
                    dbuf[b_own, sl + 1:sl + 2, :] += jnp.sum(dg, axis=0, keepdims=True)

        ag_first("V", k, du_view)

    def dx_partial(k):
        dxacc[k] = jnp.zeros_like(dxacc[k])
        if k == 0:
            for q in range(nx):
                for h in range(2):
                    lwait(("w1o", q, h))

        def use(b):
            @pl.loop(0, 2)
            def _(h):
                dxacc[k] += dot_nt(dub[2 * b + h, rows(k)], w1v[2 * b + h])

        ag_last("V", k, du_view, use)
        lcopy(("duo", k), dub.at[:, rows(k)], du_out.at[:, rows(k)])
        dxs[rows(k)] = dxacc[k].astype(BF16)
        for s in range(1, nff):
            rsend(("xr", s, k), dxs.at[q_rows(k, lax.rem(y_me + s, nff))], dxr.at[k, s - 1], ydev(s))

    def dx_sum(k):
        for s in range(1, nff):
            rwait(("xr", s, k))
        v = dxacc[k, pl.ds(pl.multiple_of(y_me * TQ, TQ), TQ)]
        for s in range(1, nff):
            v = v + dxr[k, s - 1].astype(F32)
        qr = q_rows(k, y_me)
        dxv[qr] = (ALPHA * drq[k] + v).astype(BF16)
        for s in range(1, nff):
            rsend(("xg", s, k), dxv.at[qr], dxv.at[qr], ydev(s))

    def dx_done(k):
        for s in range(1, nff):
            rwait(("xg", s, k))
        lcopy(("dxo", k), dxv.at[rows(k)], dx_out.at[rows(k)])

    def transpose_m(lo, hi):
        @pl.loop(lo, hi)
        def _(b):
            mt[b] = mb[b].T

    cs[...] = jnp.zeros_like(cs)
    dbuf[b_own] = jnp.zeros_like(dbuf[b_own])
    lwait("x")
    rwait("xx")
    u_partial(0)
    u_partial(1)
    rs_combine("U", 0, ps1, rf1, rn1)
    u_send(1, (0,))
    activate(0)
    u_send(1, (1, 2))
    xt[...] = xo[...].T
    lcopy("xto", xt, xt_out)
    ag_forward("M", 0, m_view)
    rs_combine("U", 1, ps1, rf1, rn1)
    f_partial(0)
    ln_stats(0)
    activate(1)
    ln_apply(0)
    ag_forward("M", 1, m_view)
    d_forward(0)
    dm_partial(0)
    f_partial(1)
    rs_combine("G", 0, ps2, rf2, rn2)
    ln_stats(1)
    du_make(0)
    ln_apply(1)
    for s in range(1, nff):
        rsend(("cs", s), cs, csr.at[s - 1], ydev(s))
    d_forward(1)
    dm_partial(1)
    rs_combine("G", 1, ps2, rf2, rn2)
    ag_forward("V", 0, du_view)
    transpose_m(0, nhd // 2)
    early = list(sent)
    sent.clear()
    du_make(1)
    for s in range(1, nhd):
        rsend(("db", s), dbuf.at[b_own], dbuf.at[b_own], hdev(s))
    dx_partial(0)
    transpose_m(nhd // 2, nhd)
    lcopy("mto", mt, mt_out)
    dx_sum(0)
    for cp in early:
        cp.wait_send()
    ag_forward("V", 1, du_view)
    lcopy("do", do, d_out)
    for k in range(NCHUNK):
        for s in range(1, nff):
            rwait(("y", s, k))
    lcopy("yo", yv, y_out)
    tot = cs[...]
    for s in range(1, nff):
        rwait(("cs", s))
        tot = tot + csr[s - 1]
    small_out[0:2, :] = tot[0:2, :]
    small_out[2:3, :] = jnp.sum(dyv[...].astype(F32), axis=0, keepdims=True)
    small_out[3:8, :] = jnp.zeros((5, HL), F32)
    for s in range(1, nhd):
        rwait(("db", s))
    db1_out[...] = dbuf[...]
    dx_done(0)
    dx_partial(1)
    dx_sum(1)
    dx_done(1)
    for nm in ("do", "xto", "yo", "mto"):
        lwait(nm)
    for k in range(NCHUNK):
        for nm in ("duo", "dxo"):
            lwait((nm, k))
    for cp in sent:
        cp.wait_send()


def comm_call(mesh, x, w1, b1, w2, b2, gam, bet, dy):
    nff, nhd = mesh.shape['ff'], mesh.shape['hd']
    T, HL = x.shape
    UH = w1.shape[1] // (2 * nhd)
    FB = w2.shape[0] // nhd
    FH = FB // 2
    TC = T // NCHUNK
    TQ = TC // nff
    nx = nhd // CORES
    V = pltpu.VMEM
    scratch = [
        V((T, HL), BF16), V((T, HL), BF16), V((T, HL), BF16),
        V((2 * nhd, HL, UH), BF16), V((2 * nx, HL, UH), BF16), V((nhd, FB, HL), BF16), V((nx, FB, HL), BF16),
        V((3, 2, T, UH), BF16), V((2, T, UH), BF16), V((2, 2, T, UH), BF16), V((2, T, UH), F32),
        V((3, 2, T, FH), BF16), V((2, T, FH), BF16), V((2, 2, T, FH), BF16), V((2, T, FH), F32),
        V((2, T, UH), BF16), V((nhd, T, FB), BF16), V((2 * nhd, T, UH), BF16),
        V((NCHUNK, TC, HL), F32), V((T, HL), BF16), V((NCHUNK, nff - 1, TQ, HL), BF16),
        V((NCHUNK, TQ, HL), F32), V((NCHUNK, TQ, HL), F32), V((NCHUNK, nhd, 8, 128), F32),
        V((T, HL), BF16), V((T, HL), BF16), V((T, HL), BF16),
        V((nhd, 2 * UH // 128, 128), F32), V((8, HL), F32), V((nff - 1, 8, HL), F32),
        V((NCHUNK, TC, HL), F32), V((T, HL), BF16), V((NCHUNK, nff - 1, TQ, HL), BF16), V((T, HL), BF16),
        V((nhd, FB, T), BF16), V((HL, T), BF16),
        pltpu.SemaphoreType.DMA((160,)), pltpu.SemaphoreType.DMA((160,)), pltpu.SemaphoreType.DMA((40,)),
    ]
    anyspec = pl.BlockSpec(memory_space=pl.ANY)
    vspec = pl.BlockSpec(memory_space=pltpu.VMEM)
    S = jax.ShapeDtypeStruct
    return pl.pallas_call(
        functools.partial(mlp_kernel, (nff, nhd, T, HL, UH, FB)),
        out_shape=[S((T, HL), BF16), S((T, HL), BF16), S((nhd, FB, T), BF16), S((2 * nhd, T, UH), BF16),
                   S((T, HL), BF16), S((HL, T), BF16), S((nhd, 2 * UH // 128, 128), F32), S((8, HL), F32)],
        in_specs=[anyspec, anyspec, vspec, anyspec, vspec, vspec, vspec, anyspec],
        out_specs=[anyspec, anyspec, anyspec, anyspec, anyspec, anyspec, vspec, vspec],
        scratch_shapes=scratch,
        compiler_params=pltpu.CompilerParams(collective_id=0, has_side_effects=True, vmem_limit_bytes=67043328),
        name="mlp_comm",
    )(x, w1, b1.reshape(nhd, 2 * UH // PAIR, PAIR), w2.reshape(nhd, FB, HL), b2.reshape(1, HL), gam.reshape(1, HL), bet.reshape(1, HL), dy)


def grads_kernel(xt_hbm, du_hbm, mt_hbm, d_hbm, y_hbm, dx_hbm, db1_ref, small_ref,
                 dw1_hbm, dw2_hbm, y_out, dx_out, db1_out, db2_out, dg_out, db_out,
                 xt, du, mt, d, yv, xv, o1, o2, in_sem, du_sem, mt_sem, o1_sem, o2_sem):
    n1, n2 = du.shape[0], mt.shape[0]
    UH, FB = du.shape[2], mt.shape[1]
    small = [pltpu.make_async_copy(a, b, in_sem.at[i]) for i, (a, b) in enumerate(
        ((d_hbm, d), (xt_hbm, xt), (y_hbm, yv), (dx_hbm, xv), (yv, y_out), (xv, dx_out)))]

    def du_load(i):
        return pltpu.make_async_copy(du_hbm.at[i], du.at[i], du_sem.at[i])

    def mt_load(i):
        return pltpu.make_async_copy(mt_hbm.at[i], mt.at[i], mt_sem.at[i])

    def o1_store(i):
        return pltpu.make_async_copy(o1.at[i], dw1_hbm.at[:, pl.ds(pl.multiple_of(i * UH, UH), UH)], o1_sem.at[i])

    def o2_store(i):
        return pltpu.make_async_copy(o2.at[i], dw2_hbm.at[pl.ds(pl.multiple_of(i * FB, FB), FB)], o2_sem.at[i])

    small[0].start()
    small[1].start()
    pl.loop(0, n2)(lambda i: mt_load(i).start())
    pl.loop(0, n1)(lambda i: du_load(i).start())
    small[2].start()
    small[3].start()
    db1_out[...] = db1_ref[...]
    db2_out[...] = small_ref[0:1, :]
    dg_out[...] = small_ref[1:2, :]
    db_out[...] = small_ref[2:3, :]
    small[0].wait()
    small[1].wait()

    @pl.loop(0, n2)
    def _(i):
        mt_load(i).wait()
        o2[i] = dot_nn(mt[i], d[...])
        o2_store(i).start()

    @pl.loop(0, n1)
    def _(i):
        du_load(i).wait()
        o1[i] = dot_nn(xt[...], du[i])
        o1_store(i).start()

    for i in (2, 3):
        small[i].wait()
        small[i + 2].start()
    pl.loop(0, n2)(lambda i: o2_store(i).wait())
    pl.loop(0, n1)(lambda i: o1_store(i).wait())
    for i in (4, 5):
        small[i].wait()


def weight_grads(xt, du, mt, d, y, dx, db1, small):
    n2, FB, T = mt.shape
    n1, _, UH = du.shape
    HL = xt.shape[0]
    S = jax.ShapeDtypeStruct
    V = pltpu.VMEM
    anyspec = pl.BlockSpec(memory_space=pl.ANY)
    vspec = pl.BlockSpec(memory_space=pltpu.VMEM)
    dma = pltpu.SemaphoreType.DMA
    return pl.pallas_call(
        grads_kernel,
        out_shape=[S((HL, n1 * UH), F32), S((n2 * FB, HL), F32), S(y.shape, BF16), S(dx.shape, BF16),
                   S(db1.shape, F32), S((1, HL), F32), S((1, HL), F32), S((1, HL), F32)],
        in_specs=[anyspec] * 6 + [vspec] * 2,
        out_specs=[anyspec] * 4 + [vspec] * 4,
        scratch_shapes=[V((HL, T), BF16), V((n1, T, UH), BF16), V((n2, FB, T), BF16), V((T, HL), BF16), V((T, HL), BF16), V((T, HL), BF16),
                        V((n1, HL, UH), F32), V((n2, FB, HL), F32), dma((6,)), dma((n1,)), dma((n2,)), dma((n1,)), dma((n2,))],
        compiler_params=pltpu.CompilerParams(vmem_limit_bytes=67043328),
        cost_estimate=pl.CostEstimate(flops=2 * T * HL * (n1 * UH + n2 * FB), bytes_accessed=(n1 * UH + n2 * FB) * (4 * HL + 2 * T), transcendentals=0),
        name="weight_grads",
    )(xt, du, mt, d, y, dx, db1, small)


def solution(mesh):
    data_spec = P('dp', 'hd')
    hid_spec = P('hd')
    in_specs = (data_spec, P('hd', 'ff'), P('ff'), P('ff', 'hd'), hid_spec, hid_spec, hid_spec, data_spec)
    out_specs = (data_spec, data_spec, P(('dp', 'hd'), 'ff'), P(('dp', 'ff'), 'hd'), P(('dp', 'ff')), P(('dp', 'hd')), P(('dp', 'hd')), P(('dp', 'hd')))

    def device_step(x_loc, w_up, b_up, w_down, b_down, ln_gain, ln_bias, dy_loc):
        y_loc, d_loc, mt, du, dx_loc, xt, db1, small = comm_call(
            mesh, x_loc, w_up, b_up, w_down, b_down, ln_gain, ln_bias, dy_loc)
        dw_up, dw_down, y_loc, dx_loc, db1, db2, dgain, dbias = weight_grads(xt, du, mt, d_loc, y_loc, dx_loc, db1, small)
        return (y_loc, dx_loc, dw_up, dw_down, db1.reshape(-1), db2.reshape(-1), dgain.reshape(-1), dbias.reshape(-1))

    return jax.shard_map(device_step, mesh=mesh, in_specs=in_specs, out_specs=out_specs, check_vma=False)
```
